32 devices in a mesh: pipe: 4 (over x, core), exp: 4 (over z), pair: 2 (over y).
Axes of the slice: x: 2, y: 2, z: 4, core: 2. Of those that a mesh axis runs over, the one named last changes fastest.
Arguments:
- hidden_in: bfloat16 [4, 256, 2048], P(None, ('exp', 'pair')), may hold values from -6 to 6
- routes: int32 [4, 4, 256, 8], P('pipe', None, ('exp', 'pair')), may hold values from 0 to 15, all different within a row; in each aligned block of 32 rows (0 to 31, 32 to 63, ..., all dimensions but the last counted through in order) at most 24 rows name the same one
- gate_probs: float32 [4, 4, 256, 8], P('pipe', None, ('exp', 'pair')), may hold values from 0.02 to 1
- norm_gain: float32 [4, 2048], P('pipe'), may hold values from 0.1 to 1.9
- w_gate: bfloat16 [4, 16, 2048, 768], P('pipe', ('exp', 'pair')), may hold values from -0.125 to 0.125
- w_up: bfloat16 [4, 16, 2048, 768], P('pipe', ('exp', 'pair')), may hold values from -0.125 to 0.125
- w_down: bfloat16 [4, 16, 768, 2048], P('pipe', ('exp', 'pair')), may hold values from -0.21875 to 0.21875
Outputs:
- layer_outputs: bfloat16 [4, 4, 256, 2048], P('pipe', None, ('exp', 'pair'))
The draws below stay inside these ranges and needn't reach their ends.
Inputs may be any that keep to these rules, and one draw needn't show every extreme that they name: `routes`: within each layer and micro-batch, the 32 tokens of one device (aligned blocks) name no expert more than 24 times in all, and each token names 8 different experts.
All inputs are finite; a program needn't handle non-finite values.
Results may differ from the reference program's by a relative error of at most 0.01.
Values may be sent and summed in bfloat16 or wider, within the bound.
A program may use at most 64 MiB of HBM per device.

```python
import math
import jax
import jax.numpy as jnp
import numpy as np
from jax import lax

D = 2048
FF = 768
TOPK = 8
MB = 4
TOK_DEV = 32
EXPERTS = 16
LAYERS = 4
TOKENS = 256
CAP = 24


def block_scale(rng, shape, shards, least, largest):
    def one(position, parts):
        steps = jax.random.uniform(jax.random.fold_in(jax.random.fold_in(rng, 6), position), (parts,), jnp.float32, least / len(shards), largest / len(shards))
        return jnp.repeat(jnp.exp(steps), shape[position] // parts).reshape((-1,) + (1,) * (len(shape) - position - 1))

    loudness = one(*shards[0])
    for cut in shards[1:]:
        loudness = loudness * one(*cut)
    return loudness


def routed_block(rng, own, number, rows, number_of, top, bound, skew):
    order = jax.random.permutation(rng, number_of)
    packed, common = shares(number_of, rows * top, bound, skew, True), shares(number_of, rows * top, bound, skew, False)
    places = jnp.arange(number_of)

    def named(sizes, rotation):
        used = int((sizes > 0).sum())
        fixed = max(1, used // 4)
        shifted = fixed + (places - fixed + rotation * (used - fixed)) % max(1, number_of - fixed)
        return jnp.zeros((number_of,), jnp.int32).at[order[jnp.where(places < fixed, places, shifted)]].set(jnp.asarray(sizes, jnp.int32))

    sizes = jnp.where(number % 4 == 0, named(packed, number // 4), named(common, number - number // 4 - 1))
    mixed = jax.random.permutation(jax.random.fold_in(own, 3), number_of)
    donor, taker = mixed[0:number_of // 2 * 2:2], mixed[1:number_of // 2 * 2:2]
    margin = jnp.minimum(sizes[donor] - 1, bound - sizes[taker]) // 2
    margin = jnp.where((donor == order[0]) | (taker == order[0]) | (sizes[taker] == 0), 0, jnp.maximum(margin, 0))
    shifted = jax.random.randint(jax.random.fold_in(own, 4), (number_of // 2,), 0, 1 << 20) % (margin + 1)
    sizes = sizes.at[donor].add(-shifted).at[taker].add(shifted)
    labels = jnp.searchsorted(jnp.cumsum(sizes), jnp.arange(rows * top), side="right").astype(jnp.int32)
    grid = labels.reshape(top, rows).T
    grid = grid[jax.random.permutation(jax.random.fold_in(own, 1), rows)]
    rotation = jax.random.randint(jax.random.fold_in(own, 2), (rows, 1), 0, top)
    return jnp.take_along_axis(grid, (jnp.arange(top)[None, :] + rotation) % top, axis=1)


def shares(number_of, total, most, skew, full):
    loads = [(1 << 20) // math.isqrt(grade ** skew) + 1 for grade in range(1, number_of + 1)]
    largest = most if full else min(most, max(-(-total // number_of), total * loads[0] // sum(loads)))
    least = 1 if total - largest >= number_of - 1 else 0
    counts, surplus = [largest] + [least] * (number_of - 1), total - largest - least * (number_of - 1)
    while surplus > 0:
        candidates = [i for i in range(1, number_of) if counts[i] < largest] or [i for i in range(1, number_of) if counts[i] < most]
        mass, remaining = sum([loads[i] for i in candidates]), surplus
        for i in candidates:
            addition = min(most - counts[i], max(1, remaining * loads[i] // mass), surplus)
            counts[i] = counts[i] + addition
            surplus = surplus - addition
    return np.array(counts)


def normal_values(own_key, dims, width, most, shards=(), held_as=jnp.bfloat16):
    drawn = jax.random.normal(own_key, dims, jnp.float32) * width
    if len(shards) > 0:
        drawn = block_scale(own_key, dims, shards, -0.22, 0.18) * drawn
    return jnp.clip(drawn, min=-most, max=most).astype(held_as)


def setup_inputs(seed: int = 0) -> dict:
    key_of = jax.random.split(jax.random.key(seed), 8)
    hidden_in = normal_values(key_of[0], (MB, TOKENS, D), 1.0, 6.0, ((1, 8),))
    routes_keys = jax.random.split(jax.random.fold_in(key_of[1], 1), LAYERS * MB * TOKENS // TOK_DEV)
    routes_turns = jax.random.permutation(jax.random.fold_in(key_of[1], 3), LAYERS * MB * TOKENS // TOK_DEV)
    routes = jax.vmap(lambda own, number: routed_block(jax.random.fold_in(key_of[1], 2), own, number, TOK_DEV, EXPERTS, TOPK, CAP, 2))(routes_keys, routes_turns).reshape((LAYERS, MB, TOKENS, TOPK))
    gate_probs = jnp.clip(jnp.exp(math.log(1.0) - 3.912023 * jax.random.uniform(key_of[2], (LAYERS, MB, TOKENS, TOPK), jnp.float32) ** block_scale(key_of[2], (LAYERS, MB, TOKENS, TOPK), ((0, 4), (2, 8)), -0.2, 0.2)), 0.02, 1.0)
    norm_gain = jnp.clip(1.0 + 0.18 * jax.random.normal(key_of[3], (LAYERS, D), jnp.float32), 0.1, 1.9)
    w_gate = normal_values(key_of[4], (LAYERS, EXPERTS, D, FF), D ** -0.5, 0.125, ((0, 4), (1, 8)))
    w_up = normal_values(key_of[5], (LAYERS, EXPERTS, D, FF), D ** -0.5, 0.125, ((0, 4), (1, 8)))
    w_down = normal_values(key_of[6], (LAYERS, EXPERTS, FF, D), FF ** -0.5, 0.21875, ((0, 4), (1, 8)))
    return {"hidden_in": hidden_in, "routes": routes, "gate_probs": gate_probs, "norm_gain": norm_gain, "w_gate": w_gate, "w_up": w_up, "w_down": w_down}


EPS = 1e-06

def slots_of(block_routes):
    expert_ids = jnp.arange(EXPERTS, dtype=jnp.int32)
    onehot = (block_routes[:, None] == expert_ids[None, :]).astype(jnp.int32)
    before = jnp.cumsum(onehot, axis=0) - onehot
    return lax.optimization_barrier(jnp.sum(before * onehot, axis=1)).astype(jnp.int32)

def moe_layer(state, chosen, probs, gain, wgate, wupper, wdown):
    floated = state.astype(jnp.float32)
    scale = lax.rsqrt(lax.optimization_barrier(jnp.mean(floated * floated, axis=-1, keepdims=True)) + EPS)
    normed = (floated * scale * gain.astype(jnp.float32)).astype(jnp.bfloat16)
    blocks = TOKENS // TOK_DEV
    flat_routes = chosen.reshape(blocks, TOK_DEV * TOPK).astype(jnp.int32)
    slots = jax.vmap(slots_of)(flat_routes)
    columns = (slots + CAP * jnp.arange(blocks, dtype=jnp.int32)[:, None]).reshape(-1)
    rows_ids = flat_routes.reshape(-1)
    buffer = jnp.zeros((EXPERTS, blocks * CAP, D), jnp.bfloat16)
    buffer = buffer.at[rows_ids, columns].set(jnp.repeat(normed, TOPK, axis=0))

    def one_expert(items):
        inputs, gate_w, up_w, down_w = items
        gate = jnp.dot(inputs, gate_w, preferred_element_type=jnp.float32)
        upward = jnp.dot(inputs, up_w, preferred_element_type=jnp.float32)
        hidden = (jax.nn.silu(gate) * upward).astype(jnp.bfloat16)
        return jnp.dot(hidden, down_w, preferred_element_type=jnp.float32).astype(jnp.bfloat16)
    produced = lax.map(one_expert, (buffer, wgate, wupper, wdown))
    picked = produced[rows_ids, columns].reshape(TOKENS, TOPK, D).astype(jnp.float32)
    probs32 = probs.astype(jnp.float32)
    weights = probs32 / lax.optimization_barrier(jnp.sum(probs32, axis=-1, keepdims=True))
    mixed = jnp.einsum('tk,tkd->td', weights, picked)
    return (floated + mixed).astype(jnp.bfloat16)

def reference(hidden_in, routes, gate_probs, norm_gain, w_gate, w_up, w_down):
    current = hidden_in
    outputs = []
    for layer in range(LAYERS):

        def per_batch(items):
            state, chosen, probs = items
            return moe_layer(state, chosen, probs, norm_gain[layer], w_gate[layer], w_up[layer], w_down[layer])
        current = lax.map(per_batch, (current, routes[layer], gate_probs[layer]))
        outputs.append(current)
    return jnp.stack(outputs, axis=0)
```

```python
import functools

import jax
import jax.numpy as jnp
from jax import lax
from jax.experimental import pallas as pl
from jax.experimental.pallas import tpu as pltpu
from jax.sharding import PartitionSpec as P

EPS = 1e-06
MESH = pl.DeviceIdType.MESH
F32 = jnp.float32
BF16 = jnp.bfloat16
VMEM_LIMIT = 63 * 1024 * 1024


def divisor_tile(size, most):
    tile = most
    while size % tile:
        tile //= 2
    return tile


def relay_kernel(
    stages,
    zs,
    ys,
    hidden_ref,
    routes_ref,
    probs_ref,
    gain_ref,
    wgate_ref,
    wup_ref,
    wdown_ref,
    out_ref,
    wg,
    wu,
    wd,
    hbuf,
    tokens,
    share,
    hid,
    part,
    fromy,
    zsend,
    fromz,
    obuf,
    w_sem,
    h_sem,
    hs_sem,
    o_sem,
    s_sem,
    sr_sem,
    a_sem,
    ar_sem,
    y_sem,
    yr_sem,
    z_sem,
    zr_sem,
):
    micro, rows, width = hbuf.shape
    locals_, _, ff = wg.shape
    lanes = share.shape[3]
    groups = zs * ys
    experts = groups * locals_
    stage = lax.axis_index("pipe")
    z = lax.axis_index("exp")
    y = lax.axis_index("pair")
    me = z * ys + y
    slot = y * zs + z

    def peer(dz, dy):
        return lax.rem(z + dz, zs), lax.rem(y + dy, ys)

    others = [(dz, dy) for dy in range(ys) for dz in range(zs) if dz or dy]

    loads = []
    for j in range(locals_):
        loads.append(
            (
                pltpu.make_async_copy(wgate_ref.at[0, j], wg.at[j], w_sem.at[3 * j]),
                pltpu.make_async_copy(wup_ref.at[0, j], wu.at[j], w_sem.at[3 * j + 1]),
                pltpu.make_async_copy(
                    wdown_ref.at[0, j], wd.at[pl.ds(j * ff, ff)], w_sem.at[3 * j + 2]
                ),
            )
        )

    def from_input(m):
        return pltpu.make_async_copy(hidden_ref.at[m], hbuf.at[m], h_sem.at[m])

    @pl.when(stage == 0)
    def _():
        for m in range(micro):
            from_input(m).start()

    for j in range(locals_):
        loads[j][0].start()
        loads[j][1].start()
    for j in range(locals_):
        loads[j][2].start()

    barrier = pltpu.get_barrier_semaphore()
    for dz, dy in others:
        pz, py = peer(dz, dy)
        pl.semaphore_signal(barrier, inc=1, device_id={"exp": pz, "pair": py}, device_id_type=MESH)

    @pl.when(stage > 0)
    def _():
        pl.semaphore_signal(barrier, inc=1, device_id={"pipe": stage - 1}, device_id_type=MESH)

    @pl.when(stage < stages - 1)
    def _():
        pl.semaphore_signal(barrier, inc=1, device_id={"pipe": stage + 1}, device_id_type=MESH)

    lane = lax.broadcasted_iota(jnp.int32, (rows, lanes), 1)
    for m in range(micro):
        probs = probs_ref[0, m]
        normal = probs / jnp.sum(probs, axis=-1, keepdims=True)
        chosen = routes_ref[0, m]
        total = jnp.zeros((rows, lanes), F32)
        for k in range(chosen.shape[1]):
            named = chosen[:, k : k + 1]
            hit = jnp.logical_or(lane == named, lane == named + experts)
            total = total + jnp.where(hit, normal[:, k : k + 1], 0.0)
        high = total.astype(BF16)
        low = (total - high.astype(F32)).astype(BF16)
        share[slot, m] = jnp.where(lane < experts, high, low)

    linked = (stage > 0).astype(jnp.int32) + (stage < stages - 1).astype(jnp.int32)
    pl.semaphore_wait(barrier, len(others) + linked)

    def share_copy(at, to_z, to_y):
        return pltpu.make_async_remote_copy(
            src_ref=share.at[at],
            dst_ref=share.at[at],
            send_sem=s_sem.at[to_y * zs + to_z],
            recv_sem=sr_sem.at[at],
            device_id={"exp": to_z, "pair": to_y},
            device_id_type=MESH,
        )

    def share_send():
        for dz, dy in others:
            pz, py = peer(dz, dy)
            share_copy(slot, pz, py).start()

    def share_wait():
        for dz, dy in others:
            pz, py = peer(dz, dy)
            share_copy(py * zs + pz, pz, py).wait_recv()

    def token_copy(m, at, tag, to_z, to_y):
        block = tokens.at[m, pl.ds(pl.multiple_of(at * rows, rows), rows)]
        return pltpu.make_async_remote_copy(
            src_ref=block,
            dst_ref=block,
            send_sem=a_sem.at[m, tag],
            recv_sem=ar_sem.at[m, at],
            device_id={"exp": to_z, "pair": to_y},
            device_id_type=MESH,
        )

    def y_copy(m, dy, tz):
        py = lax.rem(y + dy, ys)
        return pltpu.make_async_remote_copy(
            src_ref=part.at[m, pl.ds(pl.multiple_of((py * zs + tz) * rows, rows), rows)],
            dst_ref=fromy.at[m, dy - 1, tz],
            send_sem=y_sem.at[m, dy - 1, tz],
            recv_sem=yr_sem.at[m, dy - 1, tz],
            device_id={"pair": py},
            device_id_type=MESH,
        )

    def z_copy(m, dz):
        pz = lax.rem(z + dz, zs)
        return pltpu.make_async_remote_copy(
            src_ref=zsend.at[m, dz],
            dst_ref=fromz.at[m, dz - 1],
            send_sem=z_sem.at[m, dz - 1],
            recv_sem=zr_sem.at[m, dz - 1],
            device_id={"exp": pz},
            device_id_type=MESH,
        )

    def hand_copy(m):
        return pltpu.make_async_remote_copy(
            src_ref=obuf.at[m],
            dst_ref=hbuf.at[m],
            send_sem=hs_sem.at[m],
            recv_sem=h_sem.at[m],
            device_id={"pipe": stage + 1},
            device_id_type=MESH,
        )

    def out_copy(m):
        return pltpu.make_async_copy(obuf.at[m], out_ref.at[0, m], o_sem.at[m])

    def announce(m):
        from_input(m).wait()
        state = hbuf[m].astype(F32)
        scale = lax.rsqrt(jnp.mean(state * state, axis=-1, keepdims=True) + EPS)
        tokens[m, pl.ds(pl.multiple_of(slot * rows, rows), rows)] = (
            state * scale * gain_ref[...]
        ).astype(BF16)
        for dz in range(1, zs):
            token_copy(m, slot, dz - 1, lax.rem(z + dz, zs), y).start()
        for dy in range(1, ys):
            token_copy(m, slot, (zs - 1) + dy - 1, z, lax.rem(y + dy, ys)).start()

    nz = zs - 1

    def forward_tag(dz, dy):
        return nz + (ys - 1) + (dz - 1) * (ys - 1) + dy - 1

    def gather(m):
        for dz in range(1, zs):
            pz = lax.rem(z + dz, zs)
            at = y * zs + pz
            token_copy(m, at, dz - 1, pz, y).wait_recv()
            for dy in range(1, ys):
                token_copy(m, at, forward_tag(dz, dy), z, lax.rem(y + dy, ys)).start()
        for dy in range(1, ys):
            py = lax.rem(y + dy, ys)
            for dz in range(zs):
                pz = lax.rem(z + dz, zs)
                token_copy(m, py * zs + pz, 0, z, py).wait_recv()

    ftile = divisor_tile(ff, 256)
    ntile = divisor_tile(width, 512)
    count = groups * rows

    def compute(m):
        wide = lax.broadcasted_iota(jnp.int32, (count, lanes), 1)
        shares = share[:, m].reshape(count, lanes).astype(F32)
        for j in range(locals_):
            expert = me * locals_ + j
            mine = jnp.logical_or(wide == expert, wide == expert + experts)
            column = jnp.sum(jnp.where(mine, shares, 0.0), axis=-1, keepdims=True)

            @pl.when(m == 0)
            def _():
                loads[j][0].wait()
                loads[j][1].wait()

            for c in range(0, ff, ftile):
                gate = jnp.dot(tokens[m], wg[j, :, c : c + ftile], preferred_element_type=F32)
                upward = jnp.dot(tokens[m], wu[j, :, c : c + ftile], preferred_element_type=F32)
                hid[:, j * ff + c : j * ff + c + ftile] = (
                    jax.nn.silu(gate) * upward * column
                ).astype(BF16)

        @pl.when(m == 0)
        def _():
            for j in range(locals_):
                loads[j][2].wait()

        for c in range(0, width, ntile):
            part[m, :, c : c + ntile] = jnp.dot(
                hid[...], wd[:, c : c + ntile], preferred_element_type=F32
            ).astype(BF16)

    def own_part(m, pz):
        at = pl.multiple_of((y * zs + pz) * rows, rows)
        return part[m, pl.ds(at, rows)].astype(F32)

    def scatter(m):
        for dz in range(1, zs + 1):
            for dy in range(1, ys):
                y_copy(m, dy, lax.rem(z + dz, zs)).start()
        for dz in range(1, zs):
            pz = lax.rem(z + dz, zs)
            total = own_part(m, pz)
            for dy in range(1, ys):
                y_copy(m, dy, pz).wait_recv()
                total = total + fromy[m, dy - 1, pz].astype(F32)
            zsend[m, dz] = total.astype(BF16)
            z_copy(m, dz).start()

    def finish(m):
        total = hbuf[m].astype(F32) + own_part(m, z)
        for dy in range(1, ys):
            y_copy(m, dy, z).wait_recv()
            total = total + fromy[m, dy - 1, z].astype(F32)
        for dz in range(1, zs):
            z_copy(m, dz).wait_recv()
            total = total + fromz[m, dz - 1].astype(F32)
        obuf[m] = total.astype(BF16)

        @pl.when(stage < stages - 1)
        def _():
            hand_copy(m).start()

        out_copy(m).start()

    announce(0)
    share_send()

    @pl.loop(0, micro)
    def _(m):
        @pl.when(m > 0)
        def _():
            announce(m)

        gather(m)

        @pl.when(m == 0)
        def _():
            share_wait()

        compute(m)
        scatter(m)
        finish(m)


    for dz, dy in others:
        pz, py = peer(dz, dy)
        share_copy(slot, pz, py).wait_send()

    @pl.loop(0, micro)
    def _(m):
        for tag in range(groups - 1 + 0):
            token_copy(m, slot, tag, z, y).wait_send()
        for dy in range(1, ys):
            for tz in range(zs):
                y_copy(m, dy, tz).wait_send()
        for dz in range(1, zs):
            z_copy(m, dz).wait_send()

        @pl.when(stage < stages - 1)
        def _():
            hand_copy(m).wait_send()

        out_copy(m).wait()


def relayed(hidden_in, routes, gate_probs, norm_gain, w_gate, w_up, w_down):
    micro, rows, width = hidden_in.shape
    _, locals_, _, ff = w_gate.shape
    stages, zs, ys = (lax.axis_size(a) for a in ("pipe", "exp", "pair"))
    groups = zs * ys
    lanes = share_lanes(groups * locals_)
    dma = pltpu.SemaphoreType.DMA
    anywhere = pl.BlockSpec(memory_space=pl.ANY)
    inside = pl.BlockSpec(memory_space=pltpu.VMEM)
    return pl.pallas_call(
        functools.partial(relay_kernel, stages, zs, ys),
        out_shape=jax.ShapeDtypeStruct((1, micro, rows, width), BF16),
        in_specs=[anywhere, inside, inside, inside, anywhere, anywhere, anywhere],
        out_specs=anywhere,
        scratch_shapes=[
            pltpu.VMEM((locals_, width, ff), BF16),
            pltpu.VMEM((locals_, width, ff), BF16),
            pltpu.VMEM((locals_ * ff, width), BF16),
            pltpu.VMEM((micro, rows, width), BF16),
            pltpu.VMEM((micro, groups * rows, width), BF16),
            pltpu.VMEM((groups, micro, rows, lanes), BF16),
            pltpu.VMEM((groups * rows, locals_ * ff), BF16),
            pltpu.VMEM((micro, groups * rows, width), BF16),
            pltpu.VMEM((micro, max(1, ys - 1), zs, rows, width), BF16),
            pltpu.VMEM((micro, zs, rows, width), BF16),
            pltpu.VMEM((micro, max(1, zs - 1), rows, width), BF16),
            pltpu.VMEM((micro, rows, width), BF16),
            dma((3 * locals_,)),
            dma((micro,)),
            dma((micro,)),
            dma((micro,)),
            dma((groups,)),
            dma((groups,)),
            dma((micro, groups)),
            dma((micro, groups)),
            dma((micro, max(1, ys - 1), zs)),
            dma((micro, max(1, ys - 1), zs)),
            dma((micro, max(1, zs - 1))),
            dma((micro, max(1, zs - 1))),
        ],
        compiler_params=pltpu.CompilerParams(
            collective_id=0, has_side_effects=True, vmem_limit_bytes=VMEM_LIMIT
        ),
    )(hidden_in, routes, gate_probs, norm_gain, w_gate, w_up, w_down)


def share_lanes(experts):
    return -(-2 * experts // 128) * 128


def kernel_fits(hidden_in, w_gate, groups):
    micro, rows, width = hidden_in.shape
    _, locals_, _, ff = w_gate.shape
    weights = 3 * locals_ * width * ff
    moved = micro * rows * width * (4 * groups + 4)
    small = groups * rows * (locals_ * ff + micro * share_lanes(groups * locals_))
    fits = 2 * (weights + moved + small) + 8 * 1024 * 1024 < VMEM_LIMIT
    return fits and rows % 16 == 0 and width % 128 == 0 and ff % 128 == 0


def passed_along(value, axis, steps):
    count = lax.axis_size(axis)
    first, last = (max(0, -steps), min(count, count - steps))
    return lax.ppermute(value, axis, [(source, source + steps) for source in range(first, last)])


def expert_block(arrived, wgate, wupper, wdown):
    gate = jnp.einsum("nlcd,ldf->nlcf", arrived, wgate, preferred_element_type=jnp.float32)
    upward = jnp.einsum("nlcd,ldf->nlcf", arrived, wupper, preferred_element_type=jnp.float32)
    hidden = (jax.nn.silu(gate) * upward).astype(jnp.bfloat16)
    return jnp.einsum("nlcf,lfd->nlcd", hidden, wdown, preferred_element_type=jnp.float32).astype(
        jnp.bfloat16
    )


def on_device(hidden_in, routes, gate_probs, norm_gain, w_gate, w_up, w_down):
    if kernel_fits(hidden_in, w_gate, lax.axis_size(("exp", "pair"))):
        return relayed(hidden_in, routes, gate_probs, norm_gain, w_gate, w_up, w_down)
    section = lax.axis_index("pipe")
    micro, tok_rows, width = hidden_in.shape
    top_count = routes.shape[3]
    groups = lax.axis_size(("exp", "pair"))
    local_experts = w_gate.shape[1]
    experts = local_experts * groups
    capacity = max(2, 3 * tok_rows * top_count // (2 * experts))
    gain = norm_gain[0]
    wgate = w_gate[0]
    wupper = w_up[0]
    wdown = w_down[0]
    expert_ids = jnp.arange(experts, dtype=jnp.int32)

    def layer(state, index):
        chosen = lax.dynamic_index_in_dim(routes[0], index, 0, keepdims=False).reshape(-1)
        probs = lax.dynamic_index_in_dim(gate_probs[0], index, 0, keepdims=False)
        floated = state.astype(jnp.float32)
        scale = lax.rsqrt(jnp.mean(floated * floated, axis=-1, keepdims=True) + EPS)
        normed = (floated * scale * gain).astype(jnp.bfloat16)
        onehot = (chosen[:, None] == expert_ids[None, :]).astype(jnp.int32)
        before = jnp.cumsum(onehot, axis=0) - onehot
        slots = jnp.sum(before * onehot, axis=1)
        outgoing = jnp.zeros((experts, capacity, width), jnp.bfloat16)
        outgoing = outgoing.at[chosen, slots].set(jnp.repeat(normed, top_count, axis=0))
        grouped = outgoing.reshape(groups, local_experts, capacity, width)
        produced = expert_block(
            lax.all_to_all(grouped, ("exp", "pair"), split_axis=0, concat_axis=0, tiled=True),
            wgate,
            wupper,
            wdown,
        )
        returned = lax.all_to_all(
            produced, ("exp", "pair"), split_axis=0, concat_axis=0, tiled=True
        )
        results = returned.reshape(experts, capacity, width)[chosen, slots]
        results = results.reshape(tok_rows, top_count, width).astype(jnp.float32)
        weights = probs / jnp.sum(probs, axis=-1, keepdims=True)
        mixed = jnp.einsum("tk,tkd->td", weights, results)
        return (floated + mixed).astype(jnp.bfloat16)

    def advance(step, carry):
        received, saved = carry
        index = step - section
        valid = jnp.logical_and(index >= 0, index < micro)
        clipped = jnp.clip(index, 0, micro - 1)
        first = lax.dynamic_index_in_dim(hidden_in, clipped, 0, keepdims=False)
        state = jnp.where(section == 0, first, received)
        updated = layer(state, clipped)
        saved = jnp.where(valid, lax.dynamic_update_index_in_dim(saved, updated, clipped, 0), saved)
        received = passed_along(updated, "pipe", 1)
        return (received, saved)

    start = (
        jnp.zeros((tok_rows, width), jnp.bfloat16),
        jnp.zeros((micro, tok_rows, width), jnp.bfloat16),
    )
    received, saved = lax.fori_loop(0, micro + lax.axis_size("pipe") - 1, advance, start)
    return saved[None]


def solution(mesh):
    in_specs = (
        P(None, ("exp", "pair"), None),
        P("pipe", None, ("exp", "pair"), None),
        P("pipe", None, ("exp", "pair"), None),
        P("pipe", None),
        P("pipe", ("exp", "pair"), None, None),
        P("pipe", ("exp", "pair"), None, None),
        P("pipe", ("exp", "pair"), None, None),
    )
    out_specs = P("pipe", None, ("exp", "pair"), None)
    return jax.shard_map(
        on_device, mesh=mesh, in_specs=in_specs, out_specs=out_specs, check_vma=False
    )
```

```python
import functools

import jax
import jax.numpy as jnp
from jax import lax
from jax.experimental import pallas as pl
from jax.experimental.pallas import tpu as pltpu
from jax.sharding import PartitionSpec as P

EPS = 1e-06
MESH = pl.DeviceIdType.MESH
F32 = jnp.float32
BF16 = jnp.bfloat16
PIECES = 2
VMEM_LIMIT = 63 * 1024 * 1024


def divisor_tile(size, most):
    tile = most
    while size % tile:
        tile //= 2
    return tile


def relay_kernel(
    stages,
    zs,
    ys,
    pieces,
    hidden_ref,
    routes_ref,
    probs_ref,
    gain_ref,
    wgate_ref,
    wup_ref,
    wdown_ref,
    out_ref,
    wg,
    wu,
    wd,
    hbuf,
    tokens,
    share,
    hid,
    part,
    fromy,
    zsend,
    fromz,
    obuf,
    w_sem,
    h_sem,
    hs_sem,
    o_sem,
    s_sem,
    sr_sem,
    a_sem,
    ar_sem,
    y_sem,
    yr_sem,
    z_sem,
    zr_sem,
):
    micro, rows, width = hbuf.shape
    locals_, _, ff = wg.shape
    lanes = share.shape[3]
    groups = zs * ys
    experts = groups * locals_
    stage = lax.axis_index("pipe")
    z = lax.axis_index("exp")
    y = lax.axis_index("pair")
    me = z * ys + y
    slot = y * zs + z
    upper_half = lax.div(2 * z, zs)
    turn = 1 - 2 * upper_half

    def along(k):
        return lax.rem(z + turn * k + zs, zs)

    def peer(dz, dy):
        return lax.rem(z + dz, zs), lax.rem(y + dy, ys)

    others = [(dz, dy) for dy in range(ys) for dz in range(zs) if dz or dy]

    loads = []
    for j in range(locals_):
        loads.append(
            (
                pltpu.make_async_copy(wgate_ref.at[0, j], wg.at[j], w_sem.at[3 * j]),
                pltpu.make_async_copy(wup_ref.at[0, j], wu.at[j], w_sem.at[3 * j + 1]),
                pltpu.make_async_copy(
                    wdown_ref.at[0, j], wd.at[pl.ds(j * ff, ff)], w_sem.at[3 * j + 2]
                ),
            )
        )

    def from_input(m):
        return pltpu.make_async_copy(hidden_ref.at[m], hbuf.at[m], h_sem.at[m])

    @pl.when(stage == 0)
    def _():
        for m in range(micro):
            from_input(m).start()

    for j in range(locals_):
        loads[j][0].start()
        loads[j][1].start()
    for j in range(locals_):
        loads[j][2].start()

    barrier = pltpu.get_barrier_semaphore()
    for dz, dy in others:
        pz, py = peer(dz, dy)
        pl.semaphore_signal(barrier, inc=1, device_id={"exp": pz, "pair": py}, device_id_type=MESH)

    @pl.when(stage > 0)
    def _():
        pl.semaphore_signal(barrier, inc=1, device_id={"pipe": stage - 1}, device_id_type=MESH)

    @pl.when(stage < stages - 1)
    def _():
        pl.semaphore_signal(barrier, inc=1, device_id={"pipe": stage + 1}, device_id_type=MESH)

    lane = lax.broadcasted_iota(jnp.int32, (rows, lanes), 1)
    for m in range(micro):
        probs = probs_ref[0, m]
        normal = probs / jnp.sum(probs, axis=-1, keepdims=True)
        chosen = routes_ref[0, m]
        total = jnp.zeros((rows, lanes), F32)
        for k in range(chosen.shape[1]):
            named = chosen[:, k : k + 1]
            hit = jnp.logical_or(lane == named, lane == named + experts)
            total = total + jnp.where(hit, normal[:, k : k + 1], 0.0)
        high = total.astype(BF16)
        low = (total - high.astype(F32)).astype(BF16)
        share[slot, m] = jnp.where(lane < experts, high, low)

    linked = (stage > 0).astype(jnp.int32) + (stage < stages - 1).astype(jnp.int32)
    pl.semaphore_wait(barrier, len(others) + linked)

    def share_copy(at, to_z, to_y):
        return pltpu.make_async_remote_copy(
            src_ref=share.at[at],
            dst_ref=share.at[at],
            send_sem=s_sem.at[to_y * zs + to_z],
            recv_sem=sr_sem.at[at],
            device_id={"exp": to_z, "pair": to_y},
            device_id_type=MESH,
        )

    def share_send():
        for dz, dy in others:
            pz, py = peer(dz, dy)
            share_copy(slot, pz, py).start()

    def share_wait():
        for dz, dy in others:
            pz, py = peer(dz, dy)
            share_copy(py * zs + pz, pz, py).wait_recv()

    def token_copy(m, at, tag, to_z, to_y):
        block = tokens.at[m, pl.ds(pl.multiple_of(at * rows, rows), rows)]
        return pltpu.make_async_remote_copy(
            src_ref=block,
            dst_ref=block,
            send_sem=a_sem.at[m, tag],
            recv_sem=ar_sem.at[m, at],
            device_id={"exp": to_z, "pair": to_y},
            device_id_type=MESH,
        )

    def y_copy(m, dy, tz):
        py = lax.rem(y + dy, ys)
        return pltpu.make_async_remote_copy(
            src_ref=part.at[m, pl.ds(pl.multiple_of((py * zs + tz) * rows, rows), rows)],
            dst_ref=fromy.at[m, dy - 1, tz],
            send_sem=y_sem.at[m, dy - 1, tz],
            recv_sem=yr_sem.at[m, dy - 1, tz],
            device_id={"pair": py},
            device_id_type=MESH,
        )

    def z_copy(m, k, source):
        return pltpu.make_async_remote_copy(
            src_ref=zsend.at[m, k],
            dst_ref=fromz.at[m, source],
            send_sem=z_sem.at[m, k - 1],
            recv_sem=zr_sem.at[m, source],
            device_id={"exp": along(k)},
            device_id_type=MESH,
        )

    def hand_copy(m):
        return pltpu.make_async_remote_copy(
            src_ref=obuf.at[m],
            dst_ref=hbuf.at[m],
            send_sem=hs_sem.at[m],
            recv_sem=h_sem.at[m],
            device_id={"pipe": stage + 1},
            device_id_type=MESH,
        )

    def out_copy(m):
        return pltpu.make_async_copy(obuf.at[m], out_ref.at[0, m], o_sem.at[m])

    def announce(m):
        from_input(m).wait()
        state = hbuf[m].astype(F32)
        scale = lax.rsqrt(jnp.mean(state * state, axis=-1, keepdims=True) + EPS)
        tokens[m, pl.ds(pl.multiple_of(slot * rows, rows), rows)] = (
            state * scale * gain_ref[...]
        ).astype(BF16)
        for k in range(zs - 1, 0, -1):
            token_copy(m, slot, k - 1, along(k), y).start()
        for dy in range(1, ys):
            token_copy(m, slot, (zs - 1) + dy - 1, z, lax.rem(y + dy, ys)).start()

    nz = zs - 1

    def forward_tag(dz, dy):
        return nz + (ys - 1) + (dz - 1) * (ys - 1) + dy - 1

    def gather_z(m):
        for dz in range(1, zs):
            pz = along(dz)
            at = y * zs + pz
            token_copy(m, at, dz - 1, pz, y).wait_recv()
            for dy in range(1, ys):
                token_copy(m, at, forward_tag(dz, dy), z, lax.rem(y + dy, ys)).start()

    def gather_y(m, dy):
        py = lax.rem(y + dy, ys)
        for dz in range(zs):
            pz = lax.rem(z + dz, zs)
            token_copy(m, py * zs + pz, 0, z, py).wait_recv()

    ftile = divisor_tile(ff, 256)
    ntile = divisor_tile(width, 512)
    count = groups * rows

    def span(dy):
        return 0, pl.ds(0, count)

    def upper(m, dy):
        at, block = span(dy)
        wide = lax.broadcasted_iota(jnp.int32, (count, lanes), 1)
        shares = share[:, m].reshape(count, lanes).astype(F32)
        for j in range(locals_):
            expert = me * locals_ + j
            mine = jnp.logical_or(wide == expert, wide == expert + experts)
            column = jnp.sum(jnp.where(mine, shares, 0.0), axis=-1, keepdims=True)
            if dy == 0:

                @pl.when(m == 0)
                def _():
                    loads[j][0].wait()
                    loads[j][1].wait()

            for c in range(0, ff, ftile):
                held = tokens[m, block]
                gate = jnp.dot(held, wg[j, :, c : c + ftile], preferred_element_type=F32)
                upward = jnp.dot(held, wu[j, :, c : c + ftile], preferred_element_type=F32)
                hid[block, j * ff + c : j * ff + c + ftile] = (
                    jax.nn.silu(gate) * upward * column
                ).astype(BF16)

    def lower(m, dy):
        _, block = span(dy)
        for c in range(0, width, ntile):
            part[m, block, c : c + ntile] = jnp.dot(
                hid[block], wd[:, c : c + ntile], preferred_element_type=F32
            ).astype(BF16)

    def down_wait(m):
        @pl.when(m == 0)
        def _():
            for j in range(locals_):
                loads[j][2].wait()

    def own_part(m, pz):
        at = pl.multiple_of((y * zs + pz) * rows, rows)
        return part[m, pl.ds(at, rows)].astype(F32)

    def send_y(m, dy):
        for k in range(zs - 1, -1, -1):
            y_copy(m, dy, along(k)).start()

    def scatter(m):
        for k in range(zs - 1, 0, -1):
            pz = along(k)
            total = own_part(m, pz)
            for dy in range(1, ys):
                y_copy(m, dy, pz).wait_recv()
                total = total + fromy[m, dy - 1, pz].astype(F32)
            zsend[m, k] = total.astype(BF16)
            z_copy(m, k, z).start()

    def finish(m):
        total = hbuf[m].astype(F32) + own_part(m, z)
        for dy in range(1, ys):
            y_copy(m, dy, z).wait_recv()
            total = total + fromy[m, dy - 1, z].astype(F32)
        for k in range(1, zs):
            z_copy(m, k, along(k)).wait_recv()
            total = total + fromz[m, along(k)].astype(F32)
        obuf[m] = total.astype(BF16)

        @pl.when(stage < stages - 1)
        def _():
            hand_copy(m).start()

        out_copy(m).start()

    for i in range(pieces):
        announce(i)
    share_send()

    @pl.when(stage == 0)
    def _():
        for i in range(pieces):
            gather_z(i)

    @pl.loop(0, micro // pieces)
    def _(batch):
        m = batch * pieces
        following = m + pieces < micro
        first = jnp.logical_and(stage == 0, following)
        later = jnp.logical_and(stage > 0, following)

        @pl.when(stage > 0)
        def _():
            for i in range(pieces):
                gather_z(m + i)

        @pl.when(first)
        def _():
            for i in range(pieces):
                announce(m + pieces + i)

        @pl.when(m == 0)
        def _():
            share_wait()

        for i in range(pieces):
            for dy in range(1, ys):
                gather_y(m + i, dy)
            upper(m + i, 0)
            if i == 0:
                down_wait(m)
            lower(m + i, 0)
            for dy in range(1, ys):
                send_y(m + i, dy)

        @pl.when(first)
        def _():
            for i in range(pieces):
                gather_z(m + pieces + i)

        for i in range(pieces):
            scatter(m + i)
        for i in range(pieces):
            finish(m + i)

        @pl.when(later)
        def _():
            for i in range(pieces):
                announce(m + pieces + i)

    for dz, dy in others:
        pz, py = peer(dz, dy)
        share_copy(slot, pz, py).wait_send()

    @pl.loop(0, micro)
    def _(m):
        for tag in range(groups - 1):
            token_copy(m, slot, tag, z, y).wait_send()
        for dy in range(1, ys):
            for tz in range(zs):
                y_copy(m, dy, tz).wait_send()
        for dz in range(1, zs):
            z_copy(m, dz, z).wait_send()

        @pl.when(stage < stages - 1)
        def _():
            hand_copy(m).wait_send()

        out_copy(m).wait()


def relayed(hidden_in, routes, gate_probs, norm_gain, w_gate, w_up, w_down):
    batches, whole_rows, _ = hidden_in.shape
    pieces = PIECES if whole_rows % (16 * PIECES) == 0 else 1
    hidden_in = cut(hidden_in, 0, pieces)
    routes = cut(routes, 1, pieces)
    gate_probs = cut(gate_probs, 1, pieces)
    micro, rows, width = hidden_in.shape
    _, locals_, _, ff = w_gate.shape
    stages, zs, ys = (lax.axis_size(a) for a in ("pipe", "exp", "pair"))
    groups = zs * ys
    lanes = share_lanes(groups * locals_)
    dma = pltpu.SemaphoreType.DMA
    anywhere = pl.BlockSpec(memory_space=pl.ANY)
    inside = pl.BlockSpec(memory_space=pltpu.VMEM)
    out = pl.pallas_call(
        functools.partial(relay_kernel, stages, zs, ys, pieces),
        out_shape=jax.ShapeDtypeStruct((1, micro, rows, width), BF16),
        in_specs=[anywhere, inside, inside, inside, anywhere, anywhere, anywhere],
        out_specs=anywhere,
        scratch_shapes=[
            pltpu.VMEM((locals_, width, ff), BF16),
            pltpu.VMEM((locals_, width, ff), BF16),
            pltpu.VMEM((locals_ * ff, width), BF16),
            pltpu.VMEM((micro, rows, width), BF16),
            pltpu.VMEM((micro, groups * rows, width), BF16),
            pltpu.VMEM((groups, micro, rows, lanes), BF16),
            pltpu.VMEM((groups * rows, locals_ * ff), BF16),
            pltpu.VMEM((micro, groups * rows, width), BF16),
            pltpu.VMEM((micro, max(1, ys - 1), zs, rows, width), BF16),
            pltpu.VMEM((micro, zs, rows, width), BF16),
            pltpu.VMEM((micro, zs, rows, width), BF16),
            pltpu.VMEM((micro, rows, width), BF16),
            dma((3 * locals_,)),
            dma((micro,)),
            dma((micro,)),
            dma((micro,)),
            dma((groups,)),
            dma((groups,)),
            dma((micro, groups)),
            dma((micro, groups)),
            dma((micro, max(1, ys - 1), zs)),
            dma((micro, max(1, ys - 1), zs)),
            dma((micro, max(1, zs - 1))),
            dma((micro, zs)),
        ],
        compiler_params=pltpu.CompilerParams(
            collective_id=0, has_side_effects=True, vmem_limit_bytes=VMEM_LIMIT
        ),
    )(hidden_in, routes, gate_probs, norm_gain, w_gate, w_up, w_down)
    return out.reshape(1, batches, whole_rows, width)


def cut(value, axis, pieces):
    shape = value.shape
    rows = shape[axis + 1] // pieces
    return value.reshape(shape[:axis] + (shape[axis] * pieces, rows) + shape[axis + 2 :])


def share_lanes(experts):
    return -(-2 * experts // 128) * 128


def kernel_fits(hidden_in, w_gate, groups):
    micro, rows, width = hidden_in.shape
    _, locals_, _, ff = w_gate.shape
    weights = 3 * locals_ * width * ff
    moved = micro * rows * width * (4 * groups + 5)
    small = groups * rows * (locals_ * ff + micro * share_lanes(groups * locals_))
    fits = 2 * (weights + moved + small) + 8 * 1024 * 1024 < VMEM_LIMIT
    return fits and rows % 16 == 0 and width % 128 == 0 and ff % 128 == 0


def passed_along(value, axis, steps):
    count = lax.axis_size(axis)
    first, last = (max(0, -steps), min(count, count - steps))
    return lax.ppermute(value, axis, [(source, source + steps) for source in range(first, last)])


def expert_block(arrived, wgate, wupper, wdown):
    gate = jnp.einsum("nlcd,ldf->nlcf", arrived, wgate, preferred_element_type=jnp.float32)
    upward = jnp.einsum("nlcd,ldf->nlcf", arrived, wupper, preferred_element_type=jnp.float32)
    hidden = (jax.nn.silu(gate) * upward).astype(jnp.bfloat16)
    return jnp.einsum("nlcf,lfd->nlcd", hidden, wdown, preferred_element_type=jnp.float32).astype(
        jnp.bfloat16
    )


def on_device(hidden_in, routes, gate_probs, norm_gain, w_gate, w_up, w_down):
    if kernel_fits(hidden_in, w_gate, lax.axis_size(("exp", "pair"))):
        return relayed(hidden_in, routes, gate_probs, norm_gain, w_gate, w_up, w_down)
    section = lax.axis_index("pipe")
    micro, tok_rows, width = hidden_in.shape
    top_count = routes.shape[3]
    groups = lax.axis_size(("exp", "pair"))
    local_experts = w_gate.shape[1]
    experts = local_experts * groups
    capacity = max(2, 3 * tok_rows * top_count // (2 * experts))
    gain = norm_gain[0]
    wgate = w_gate[0]
    wupper = w_up[0]
    wdown = w_down[0]
    expert_ids = jnp.arange(experts, dtype=jnp.int32)

    def layer(state, index):
        chosen = lax.dynamic_index_in_dim(routes[0], index, 0, keepdims=False).reshape(-1)
        probs = lax.dynamic_index_in_dim(gate_probs[0], index, 0, keepdims=False)
        floated = state.astype(jnp.float32)
        scale = lax.rsqrt(jnp.mean(floated * floated, axis=-1, keepdims=True) + EPS)
        normed = (floated * scale * gain).astype(jnp.bfloat16)
        onehot = (chosen[:, None] == expert_ids[None, :]).astype(jnp.int32)
        before = jnp.cumsum(onehot, axis=0) - onehot
        slots = jnp.sum(before * onehot, axis=1)
        outgoing = jnp.zeros((experts, capacity, width), jnp.bfloat16)
        outgoing = outgoing.at[chosen, slots].set(jnp.repeat(normed, top_count, axis=0))
        grouped = outgoing.reshape(groups, local_experts, capacity, width)
        produced = expert_block(
            lax.all_to_all(grouped, ("exp", "pair"), split_axis=0, concat_axis=0, tiled=True),
            wgate,
            wupper,
            wdown,
        )
        returned = lax.all_to_all(
            produced, ("exp", "pair"), split_axis=0, concat_axis=0, tiled=True
        )
        results = returned.reshape(experts, capacity, width)[chosen, slots]
        results = results.reshape(tok_rows, top_count, width).astype(jnp.float32)
        weights = probs / jnp.sum(probs, axis=-1, keepdims=True)
        mixed = jnp.einsum("tk,tkd->td", weights, results)
        return (floated + mixed).astype(jnp.bfloat16)

    def advance(step, carry):
        received, saved = carry
        index = step - section
        valid = jnp.logical_and(index >= 0, index < micro)
        clipped = jnp.clip(index, 0, micro - 1)
        first = lax.dynamic_index_in_dim(hidden_in, clipped, 0, keepdims=False)
        state = jnp.where(section == 0, first, received)
        updated = layer(state, clipped)
        saved = jnp.where(valid, lax.dynamic_update_index_in_dim(saved, updated, clipped, 0), saved)
        received = passed_along(updated, "pipe", 1)
        return (received, saved)

    start = (
        jnp.zeros((tok_rows, width), jnp.bfloat16),
        jnp.zeros((micro, tok_rows, width), jnp.bfloat16),
    )
    received, saved = lax.fori_loop(0, micro + lax.axis_size("pipe") - 1, advance, start)
    return saved[None]


def solution(mesh):
    in_specs = (
        P(None, ("exp", "pair"), None),
        P("pipe", None, ("exp", "pair"), None),
        P("pipe", None, ("exp", "pair"), None),
        P("pipe", None),
        P("pipe", ("exp", "pair"), None, None),
        P("pipe", ("exp", "pair"), None, None),
        P("pipe", ("exp", "pair"), None, None),
    )
    out_specs = P("pipe", None, ("exp", "pair"), None)
    return jax.shard_map(
        on_device, mesh=mesh, in_specs=in_specs, out_specs=out_specs, check_vma=False
    )
```
